32 devices in a mesh: shift: 8 (over y, x, core), dom: 4 (over z).
Axes of the slice: x: 2, y: 2, z: 4, core: 2. Of those that a mesh axis runs over, the one named last changes fastest.
Arguments:
- samples: float32 [32, 64, 1024], P('dom'), may hold values from -6 to 6
- potential: float32 [32, 1024], P('dom'), may hold values from 0 to 4
Outputs:
- subspace: float32 [32, 64, 1024], P('dom')
- reduced_h: float32 [64, 64], replicated
- reduced_b: float32 [64, 64], replicated
The draws below stay inside these ranges and needn't reach their ends.
All inputs are finite; a program needn't handle non-finite values.
Results may differ from the reference program's by a relative error of at most 0.00027.
Values sent between devices are 32-bit elements; how exact they have to be, the bound alone decides.
No kernel may reach another device: no remote copies, remote signals or barrier semaphores. Data moves between devices by JAX's collectives and lax.ppermute only.
A program may use at most 128 MiB of HBM per device.

```python
import math
import jax
import jax.numpy as jnp
from jax import lax

NV = 64
NX = 32
NY = 32
NZ = 32
NXY = 1024
SHIFTS = 8


def block_levels(stream_key, shape, cuts, least, high):
    loudness, own = 1.0, jax.random.fold_in(stream_key, 6)
    for axis_at, shards_of in cuts:
        steps = jnp.exp(jax.random.uniform(jax.random.fold_in(own, axis_at), (shards_of,), jnp.float32, least / len(cuts), high / len(cuts)))
        loudness = loudness * jnp.repeat(steps, shape[axis_at] // shards_of).reshape([-1 if axis == axis_at else 1 for axis in range(len(shape))])
    return loudness


def normal_values(key, shape, deviation, limit, shards=(), kind=jnp.bfloat16):
    entries = jax.random.normal(key, shape, jnp.float32) * deviation
    if len(shards) > 0:
        entries = block_levels(key, shape, shards, -0.22, 0.18) * entries
    return jnp.clip(entries, min=-limit, max=limit).astype(kind)


def setup_inputs(seed: int = 0) -> dict:
    splits = jax.random.split(jax.random.key(seed), 3)
    return {
        "samples": normal_values(splits[0], (NZ, NV, NXY), 1.0, 6.0, ((0, 4),), jnp.float32),
        "potential": jnp.clip(4.0 * jax.random.uniform(splits[1], (NZ, NXY), jnp.float32) ** block_levels(splits[1], (NZ, NXY), ((0, 4),), -0.2, 0.2), 0.0, 4.0),
    }


CENTRE = 3.0
RADIUS = 2.0
RIDGE = 0.01


def plane_sum(values):
    grid = values.reshape(values.shape[:-1] + (NX, NY))
    padded = jnp.pad(grid, [(0, 0)] * (values.ndim - 1) + [(1, 1), (1, 1)])
    total = padded[..., 2:, 1:-1] + padded[..., :-2, 1:-1] + padded[..., 1:-1, 2:] + padded[..., 1:-1, :-2]
    return total.reshape(values.shape)


def hamiltonian(values, onsite):
    padded = jnp.pad(values, [(1, 1)] + [(0, 0)] * (values.ndim - 1))
    return onsite * values - (padded[2:] + padded[:-2] + plane_sum(values))


def colsum(values):
    return jnp.sum(values, axis=(0, 2))


def reference(samples, potential):
    onsite = (6.0 + potential)[:, None, :]
    moment = jnp.zeros(samples.shape, jnp.float32)
    for order in range(SHIFTS):
        angle = math.pi * (order + 0.5) / SHIFTS
        shift_re = CENTRE + RADIUS * math.cos(angle)
        shift_im = RADIUS * math.sin(angle)
        weight_re = RADIUS * math.cos(angle) / SHIFTS
        weight_im = RADIUS * math.sin(angle) / SHIFTS
        diag_re = shift_re - onsite
        modulus = diag_re * diag_re + shift_im * shift_im
        inv_re = diag_re / modulus
        inv_im = -shift_im / modulus

        def preconditioning_operator(real_part, imag_part):
            return real_part * inv_re - imag_part * inv_im, real_part * inv_im + imag_part * inv_re

        def operate(real_part, imag_part):
            ham_re = hamiltonian(real_part, onsite)
            ham_im = hamiltonian(imag_part, onsite)
            return (shift_re * real_part - shift_im * imag_part - ham_re,
                    shift_re * imag_part + shift_im * real_part - ham_im)

        first_block_real, first_block_imag = operate(samples * inv_re, samples * inv_im)
        two_re, two_im = operate(*preconditioning_operator(first_block_real, first_block_imag))
        g_one = colsum(first_block_real * first_block_real + first_block_imag * first_block_imag)
        q_one_re = colsum(first_block_real * samples)
        q_one_im = colsum(-first_block_imag * samples)
        g_mix_re = colsum(first_block_real * two_re + first_block_imag * two_im)
        g_mix_im = colsum(first_block_real * two_im - first_block_imag * two_re)
        g_two = colsum(two_re * two_re + two_im * two_im)
        q_two_re = colsum(two_re * samples)
        q_two_im = colsum(-two_im * samples)
        ridge = RIDGE * (g_one + g_two) / 2.0
        determ = (g_one + ridge) * (g_two + ridge) - (g_mix_re * g_mix_re + g_mix_im * g_mix_im)
        coef_one_re = ((g_two + ridge) * q_one_re - (g_mix_re * q_two_re - g_mix_im * q_two_im)) / determ
        coef_one_im = ((g_two + ridge) * q_one_im - (g_mix_re * q_two_im + g_mix_im * q_two_re)) / determ
        coef_two_re = ((g_one + ridge) * q_two_re - (g_mix_re * q_one_re + g_mix_im * q_one_im)) / determ
        coefficient_second_imag = ((g_one + ridge) * q_two_im - (g_mix_re * q_one_im - g_mix_im * q_one_re)) / determ
        first_coefficient_real = coef_one_re[None, :, None]
        first_coefficient_imag = coef_one_im[None, :, None]
        second_coefficient_real = coef_two_re[None, :, None]
        second_coefficient_imag = coefficient_second_imag[None, :, None]
        solved_real_part, solved_imag_part = preconditioning_operator(first_coefficient_real * samples + second_coefficient_real * first_block_real - second_coefficient_imag * first_block_imag,
                                 first_coefficient_imag * samples + second_coefficient_real * first_block_imag + second_coefficient_imag * first_block_real)
        moment = moment + (weight_re * solved_real_part - weight_im * solved_imag_part)
    scale = 1.0 / (NX * NY * NZ)
    applied = hamiltonian(moment, onsite)
    reduced_h = jnp.einsum('znc,zmc->nm', moment, applied, precision=lax.Precision.HIGHEST) * scale
    reduced_b = jnp.einsum('znc,zmc->nm', moment, moment, precision=lax.Precision.HIGHEST) * scale
    return moment, reduced_h, reduced_b
```

```python
import functools
import math

import jax
import jax.numpy as jnp
from jax import lax
from jax.experimental import pallas as pl
from jax.experimental.pallas import tpu as pltpu
from jax.sharding import PartitionSpec as P

NX = 32
NY = 32
LANES = 128


CENTRE = 3.0
RADIUS = 2.0
RIDGE = 0.01
PRODUCTS = 8


def lane_iota(rows):
    return lax.broadcasted_iota(jnp.int32, (rows, LANES), 1)


def split(ref_row):
    return [ref_row[:, j * LANES : (j + 1) * LANES] for j in range(ref_row.shape[-1] // LANES)]


def strided_order(parts):
    count = len(parts)
    blocks = LANES // NY
    lane_block = lane_iota(parts[0].shape[0]) // NY
    out = []
    for j in range(count):
        total = None
        for b in range(blocks):
            x = b * count + j
            turn = (NY * (b - x % blocks)) % LANES
            piece = parts[x // blocks]
            piece = pltpu.roll(piece, turn, 1) if turn else piece
            total = piece if total is None else jnp.where(lane_block == b, piece, total)
        out.append(total)
    return out


def natural_order(parts):
    count = len(parts)
    blocks = LANES // NY
    lane_block = lane_iota(parts[0].shape[0]) // NY
    out = []
    for v in range(count):
        total = None
        for c in range(blocks):
            x = v * blocks + c
            turn = (NY * (c - x // count)) % LANES
            piece = parts[x % count]
            piece = pltpu.roll(piece, turn, 1) if turn else piece
            total = piece if total is None else jnp.where(lane_block == c, piece, total)
        out.append(total)
    return out


def plane_neighbours(parts):
    count = len(parts)
    lane = lane_iota(parts[0].shape[0])
    has_low = (lane % NY != 0).astype(jnp.float32)
    has_high = (lane % NY != NY - 1).astype(jnp.float32)
    first = jnp.where(lane < NY, 0.0, pltpu.roll(parts[-1], NY, 1))
    last = jnp.where(lane >= LANES - NY, 0.0, pltpu.roll(parts[0], LANES - NY, 1))
    padded = [first] + parts + [last]
    return [
        padded[j] + padded[j + 2]
        + pltpu.roll(parts[j], 1, 1) * has_low
        + pltpu.roll(parts[j], LANES - 1, 1) * has_high
        for j in range(count)
    ]


def inverses(onsite, shift_re, shift_im):
    diag_re = shift_re - onsite
    scaled = 1.0 / (diag_re * diag_re + shift_im * shift_im)
    return diag_re * scaled, -shift_im * scaled


def krylov_kernel(where, nodes_ref, own, pot, low, high, blocks, b_ref, wide, sums, u, v, inv, onsite):
    k = pl.program_id(0)
    count = pl.num_programs(0)
    planes, cols, cells = own.shape
    vecs = cells // LANES

    @pl.when(k == 0)
    def _():
        sums[...] = jnp.zeros_like(sums)

        def put(z, parts):
            for j, part in enumerate(strided_order(parts)):
                b_ref[z, :, j * LANES : (j + 1) * LANES] = part

        for i in range(2):
            put(i, split(low[i * cols : (i + 1) * cols, :]))
            put(planes + 2 + i, split(high[i * cols : (i + 1) * cols, :]))

        @pl.loop(0, planes)
        def _(z):
            put(z + 2, split(own[z]))

        for start, rows in ((0, low[2 * cols :, :]), (2, pot[...]), (planes + 2, high[2 * cols :, :])):
            for j, part in enumerate(strided_order(split(rows))):
                onsite[start : start + rows.shape[0], j * LANES : (j + 1) * LANES] = 6.0 + part
        for z in range(planes + 4):
            wide[z] = jnp.broadcast_to(onsite[z : z + 1, :], (cols, cells))

    inv_re, inv_im = inverses(onsite[...], nodes_ref[k, 0], nodes_ref[k, 1])
    for z in range(planes + 4):
        inv[0, z] = jnp.broadcast_to(inv_re[z : z + 1], (cols, cells))
        inv[1, z] = jnp.broadcast_to(inv_im[z : z + 1], (cols, cells))

    def at(j):
        return slice(j * LANES, (j + 1) * LANES)

    def factor(c, z, j):
        return inv[c, z, :, at(j)]

    @pl.loop(0, planes + 4)
    def _(z):
        for j in range(vecs):
            value = b_ref[z, :, at(j)]
            u[0, z, :, at(j)] = value * factor(0, z, j)
            u[1, z, :, at(j)] = value * factor(1, z, j)

    def image(field, c, z):
        beside = plane_neighbours([field[c, z, :, at(j)] for j in range(vecs)])
        return [beside[j] + (field[c, z - 1, :, at(j)] + field[c, z + 1, :, at(j)]) for j in range(vecs)]

    @pl.loop(0, planes + 2)
    def _(z):
        low_in = where[1].astype(jnp.float32)
        high_in = where[2].astype(jnp.float32)
        inside = jnp.where(z == 0, low_in, jnp.where(z == planes + 1, high_in, 1.0))
        real = image(u, 0, z + 1)
        imag = image(u, 1, z + 1)
        for j in range(vecs):
            re = (b_ref[z + 1, :, at(j)] + real[j]) * inside
            im = imag[j] * inside
            f_re = factor(0, z + 1, j)
            f_im = factor(1, z + 1, j)
            blocks[0, 0, z, :, at(j)] = re
            blocks[0, 1, z, :, at(j)] = im
            v[0, z, :, at(j)] = re * f_re - im * f_im
            v[1, z, :, at(j)] = re * f_im + im * f_re

    def accumulate(z, acc):
        real = image(v, 0, z + 1)
        imag = image(v, 1, z + 1)
        acc = list(acc)
        for j in range(vecs):
            re = blocks[0, 0, z + 1, :, at(j)]
            im = blocks[0, 1, z + 1, :, at(j)]
            two_re = re + real[j]
            two_im = im + imag[j]
            b = b_ref[z + 2, :, at(j)]
            acc[0] = acc[0] + (re * re + im * im)
            acc[1] = acc[1] + re * b
            acc[2] = acc[2] - im * b
            acc[3] = acc[3] + (re * two_re + im * two_im)
            acc[4] = acc[4] + (re * two_im - im * two_re)
            acc[5] = acc[5] + (two_re * two_re + two_im * two_im)
            acc[6] = acc[6] + two_re * b
            acc[7] = acc[7] - two_im * b
        return tuple(acc)

    zero = jnp.zeros((cols, LANES), jnp.float32)
    acc = lax.fori_loop(0, planes, accumulate, (zero,) * PRODUCTS)
    lane = lane_iota(cols)
    total = sums[...]
    for i in range(PRODUCTS):
        total = jnp.where(lane == i * count + k, jnp.sum(acc[i], axis=1, keepdims=True), total)
    sums[...] = total


def moment_kernel(shifts, weights, blocks, b_ref, onsite, sums, out, coef):
    z = pl.program_id(0)
    nodes = blocks.shape[0]
    cols, cells = b_ref.shape[1:]
    vecs = cells // LANES

    @pl.when(z == 0)
    def _():
        total = sums[...]

        def of(i):
            return pltpu.roll(total, (LANES - i * nodes) % LANES, 1) if i else total

        g_one, q_one_re, q_one_im, g_mix_re, g_mix_im, g_two, q_two_re, q_two_im = map(of, range(PRODUCTS))
        ridge = RIDGE * (g_one + g_two) / 2.0
        determ = (g_one + ridge) * (g_two + ridge) - (g_mix_re * g_mix_re + g_mix_im * g_mix_im)
        one_re = ((g_two + ridge) * q_one_re - (g_mix_re * q_two_re - g_mix_im * q_two_im)) / determ
        one_im = ((g_two + ridge) * q_one_im - (g_mix_re * q_two_im + g_mix_im * q_two_re)) / determ
        two_re = ((g_one + ridge) * q_two_re - (g_mix_re * q_one_re + g_mix_im * q_one_im)) / determ
        two_im = ((g_one + ridge) * q_two_im - (g_mix_re * q_one_im - g_mix_im * q_one_re)) / determ
        w_re = weights[0:1, :]
        w_im = weights[1:2, :]
        scaled = (
            w_re * one_re - w_im * one_im,
            w_re * one_im + w_im * one_re,
            w_re * two_re - w_im * two_im,
            w_re * two_im + w_im * two_re,
        )
        for k in range(nodes):
            for i in range(4):
                coef[k, i] = jnp.broadcast_to(scaled[i][:, k : k + 1], (cols, LANES))

    result = []
    for j in range(vecs):
        at = slice(j * LANES, (j + 1) * LANES)
        b = b_ref[z + 2, :, at]
        total = jnp.zeros((cols, LANES), jnp.float32)
        inv_re, inv_im = inverses(onsite[z + 2, 0:1, at], shifts[0], shifts[1])
        for k in range(nodes):
            re = blocks[k, 0, 0, :, at]
            im = blocks[k, 1, 0, :, at]
            f_re = jnp.broadcast_to(inv_re[k : k + 1], (cols, LANES))
            f_im = jnp.broadcast_to(inv_im[k : k + 1], (cols, LANES))
            y_re = coef[k, 0] * b + coef[k, 2] * re - coef[k, 3] * im
            y_im = coef[k, 1] * b + coef[k, 3] * re + coef[k, 2] * im
            total = total + (f_re * y_re - f_im * y_im)
        result.append(total)
    for j, part in enumerate(natural_order(result)):
        out[0, :, j * LANES : (j + 1) * LANES] = part


def halves(x):
    high = x.astype(jnp.bfloat16)
    return high, (x - high.astype(jnp.float32)).astype(jnp.bfloat16)


def gram_kernel(where, pot, *refs, layout, scale):
    pieces, out, gram, edge = refs[: len(layout)], refs[-3], refs[-2], refs[-1]
    planes, width, cells = out.shape
    for ref, (mask, first) in zip(pieces, layout):
        cols = ref.shape[1]
        start = 0 if cols == width else pl.multiple_of((where[0] ^ mask) * cols, cols)
        for z in range(ref.shape[0]):
            if first + z < planes:
                out[first + z, pl.ds(start, cols), :] = ref[z]
            else:
                edge[pl.ds(start, cols), :] = ref[z]
    cell = lax.broadcasted_iota(jnp.int32, (1, cells), 1)
    x_ok = (cell < cells - NY).astype(jnp.float32)
    y_ok = (cell % NY != NY - 1).astype(jnp.float32)
    total = jnp.zeros((2 * width, 4 * width), jnp.float32)
    for z in range(planes):
        s = out[z]
        after = out[z + 1] if z + 1 < planes else edge[...]
        beside = pltpu.roll(s, cells - NY, 1) * x_ok + pltpu.roll(s, cells - 1, 1) * y_ok + after
        applied = (3.0 + 0.5 * pot[z : z + 1, :]) * s - beside
        s_high, s_low = halves(s)
        a_high, a_low = halves(applied)
        left = jnp.concatenate([s_high, s_low], axis=0)
        right = jnp.concatenate([a_high, s_high, a_low, s_low], axis=0)
        total = total + lax.dot_general(
            left, right, (((1,), (1,)), ((), ())), preferred_element_type=jnp.float32
        )
    both = total[:width, : 2 * width] + total[:width, 2 * width :] + total[width:, : 2 * width]
    gram[...] = both * scale


def butterfly(x, axis):
    count = lax.axis_size(axis)
    step = 1
    while step < count:
        x = x + lax.ppermute(x, axis, [(i, i ^ step) for i in range(count)])
        step *= 2
    return x


def swap(x, mask):
    count = lax.axis_size("shift")
    return lax.ppermute(x, "shift", [(i, i ^ mask) for i in range(count)])


def spread(x):
    count = lax.axis_size("shift")
    if x.shape[1] % 8:
        whole = lax.all_gather(x, "shift", axis=1)
        return [(0, 0, whole.reshape(x.shape[0], -1, x.shape[2]))]
    if count != 8:
        return [(0, 0, x)] + [(m, 0, swap(x, m)) for m in range(1, count)]
    half = x.shape[0] // 2
    a = swap(x, 2)
    b = swap(x, 4)
    d_first = swap(a[:half], 4)
    d_last = swap(b[half:], 2)
    held = [(0, 0, x), (2, 0, a), (4, 0, b), (6, 0, d_first), (6, half, d_last)]
    return held + [(m ^ 1, first, swap(piece, 1)) for m, first, piece in held]


def on_device(samples, potential):
    nodes = lax.axis_size("shift")
    slabs = lax.axis_size("dom")
    planes, width, cells = samples.shape
    cols = width // nodes
    me = lax.axis_index("shift")
    slab = lax.axis_index("dom")
    angles = [math.pi * (k + 0.5) / nodes for k in range(nodes)]
    table = jnp.array(
        [[CENTRE + RADIUS * math.cos(a), RADIUS * math.sin(a)] for a in angles], jnp.float32
    )
    shifts = jnp.broadcast_to(table.T[:, :, None], (2, nodes, LANES))
    spare = [0.0] * (LANES - nodes)
    weights = jnp.array(
        [
            [RADIUS * math.cos(a) / nodes for a in angles] + spare,
            [RADIUS * math.sin(a) / nodes for a in angles] + spare,
        ],
        jnp.float32,
    )
    where = jnp.stack([me, slab > 0, slab < slabs - 1]).astype(jnp.int32)

    def edge(start):
        part = lax.dynamic_slice(samples, (start, me * cols, 0), (2, cols, cells))
        return jnp.concatenate([part.reshape(2 * cols, cells), potential[start : start + 2]], axis=0)

    up = [(i, i + 1) for i in range(slabs - 1)]
    down = [(j, i) for i, j in up]
    low = lax.ppermute(edge(planes - 2), "dom", up)
    high = lax.ppermute(edge(0), "dom", down)

    f32 = jnp.float32
    smem = pl.BlockSpec(memory_space=pltpu.SMEM)

    def full(shape):
        return pl.BlockSpec(shape, lambda *_: (0,) * len(shape))

    if cols % 8:
        source = lax.dynamic_slice_in_dim(samples, me * cols, cols, 1)
        own_spec = full(source.shape)
    else:
        source = samples
        own_spec = pl.BlockSpec((planes, cols, cells), lambda k, w: (0, w[0], 0))
    blocks, b_ext, onsite, sums = pl.pallas_call(
        krylov_kernel,
        grid_spec=pltpu.PrefetchScalarGridSpec(
            num_scalar_prefetch=1,
            grid=(nodes,),
            in_specs=[
                smem,
                own_spec,
                full(potential.shape),
                full(low.shape),
                full(high.shape),
            ],
            out_specs=[
                pl.BlockSpec((1, 2, planes + 2, cols, cells), lambda k, w: (k, 0, 0, 0, 0)),
                full((planes + 4, cols, cells)),
                full((planes + 4, cols, cells)),
                full((cols, LANES)),
            ],
            scratch_shapes=[
                pltpu.VMEM((2, planes + 4, cols, cells), f32),
                pltpu.VMEM((2, planes + 2, cols, cells), f32),
                pltpu.VMEM((2, planes + 4, cols, cells), f32),
                pltpu.VMEM((planes + 4, cells), f32),
            ],
        ),
        out_shape=[
            jax.ShapeDtypeStruct((nodes, 2, planes + 2, cols, cells), f32),
            jax.ShapeDtypeStruct((planes + 4, cols, cells), f32),
            jax.ShapeDtypeStruct((planes + 4, cols, cells), f32),
            jax.ShapeDtypeStruct((cols, LANES), f32),
        ],
        name="krylov",
    )(where, table, source, potential, low, high)

    totals = butterfly(sums, "dom")

    own = pl.pallas_call(
        moment_kernel,
        grid=(planes + 1,),
        in_specs=[
            full(shifts.shape),
            full(weights.shape),
            pl.BlockSpec((nodes, 2, 1, cols, cells), lambda z: (0, 0, z + 1, 0, 0)),
            full(b_ext.shape),
            full(onsite.shape),
            full(totals.shape),
        ],
        out_specs=pl.BlockSpec((1, cols, cells), lambda z: (z, 0, 0)),
        out_shape=jax.ShapeDtypeStruct((planes + 1, cols, cells), f32),
        scratch_shapes=[
            pltpu.VMEM((nodes, 4, cols, LANES), f32),
        ],
        name="moment",
    )(shifts, weights, blocks, b_ext, onsite, totals)

    held = spread(own)
    layout = tuple((mask, first) for mask, first, _ in held)
    vmem = pl.BlockSpec(memory_space=pltpu.VMEM)
    scale = 1.0 / (cells * planes * slabs)
    subspace, gram = pl.pallas_call(
        functools.partial(gram_kernel, layout=layout, scale=scale),
        in_specs=[smem] + [vmem] * (1 + len(held)),
        out_specs=[vmem, vmem],
        out_shape=[
            jax.ShapeDtypeStruct((planes, width, cells), f32),
            jax.ShapeDtypeStruct((width, 2 * width), f32),
        ],
        scratch_shapes=[pltpu.VMEM((width, cells), f32)],
        name="gram",
    )(where, potential, *[piece for _, _, piece in held])
    gram = butterfly(gram, "dom")
    part_h = gram[:, :width]
    return subspace, part_h + part_h.T, gram[:, width:]


def solution(mesh):
    in_specs = (P("dom", None, None), P("dom", None))
    out_specs = (P("dom", None, None), P(), P())
    return jax.shard_map(
        on_device, mesh=mesh, in_specs=in_specs, out_specs=out_specs, check_vma=False
    )
```

```python
import functools
import math

import jax
import jax.numpy as jnp
import numpy as np
from jax import lax
from jax.experimental import pallas as pl
from jax.experimental.pallas import tpu as pltpu
from jax.sharding import PartitionSpec as P

NX = 32
NY = 32
LANES = 128


CENTRE = 3.0
RADIUS = 2.0
RIDGE = 0.01
PRODUCTS = 8


def lane_iota(rows):
    return lax.broadcasted_iota(jnp.int32, (rows, LANES), 1)


def split(ref_row):
    return [ref_row[:, j * LANES : (j + 1) * LANES] for j in range(ref_row.shape[-1] // LANES)]


def strided_order(parts):
    count = len(parts)
    blocks = LANES // NY
    lane_block = lane_iota(parts[0].shape[0]) // NY
    out = []
    for j in range(count):
        total = None
        for b in range(blocks):
            x = b * count + j
            turn = (NY * (b - x % blocks)) % LANES
            piece = parts[x // blocks]
            piece = pltpu.roll(piece, turn, 1) if turn else piece
            total = piece if total is None else jnp.where(lane_block == b, piece, total)
        out.append(total)
    return out


def natural_order(parts):
    count = len(parts)
    blocks = LANES // NY
    lane_block = lane_iota(parts[0].shape[0]) // NY
    out = []
    for v in range(count):
        total = None
        for c in range(blocks):
            x = v * blocks + c
            turn = (NY * (c - x // count)) % LANES
            piece = parts[x % count]
            piece = pltpu.roll(piece, turn, 1) if turn else piece
            total = piece if total is None else jnp.where(lane_block == c, piece, total)
        out.append(total)
    return out


def plane_neighbours(parts):
    count = len(parts)
    lane = lane_iota(parts[0].shape[0])
    has_low = (lane % NY != 0).astype(jnp.float32)
    has_high = (lane % NY != NY - 1).astype(jnp.float32)
    first = jnp.where(lane < NY, 0.0, pltpu.roll(parts[-1], NY, 1))
    last = jnp.where(lane >= LANES - NY, 0.0, pltpu.roll(parts[0], LANES - NY, 1))
    padded = [first] + parts + [last]
    return [
        padded[j] + padded[j + 2]
        + pltpu.roll(parts[j], 1, 1) * has_low
        + pltpu.roll(parts[j], LANES - 1, 1) * has_high
        for j in range(count)
    ]


def inverses(onsite, shift_re, shift_im):
    diag_re = shift_re - onsite
    scaled = 1.0 / (diag_re * diag_re + shift_im * shift_im)
    return diag_re * scaled, -shift_im * scaled


def krylov_kernel(where, nodes_ref, own, pot, paired, other, blocks, b_ref, wide, sums, u, v, inv, onsite):
    k = pl.program_id(0)
    count = pl.num_programs(0)
    planes, cols, cells = own.shape
    vecs = cells // LANES

    @pl.when(k == 0)
    def _():
        sums[...] = jnp.zeros_like(sums)

        def put(z, parts):
            for j, part in enumerate(strided_order(parts)):
                b_ref[z, :, j * LANES : (j + 1) * LANES] = part

        even = where[3] > 0
        low = jnp.where(even, other[...], paired[...])
        high = jnp.where(even, paired[...], other[...])
        for i in range(2):
            put(i, split(low[i * cols : (i + 1) * cols, :]))
            put(planes + 2 + i, split(high[i * cols : (i + 1) * cols, :]))

        @pl.loop(0, planes)
        def _(z):
            put(z + 2, split(own[z]))

        for start, rows in ((0, low[2 * cols :, :]), (2, pot[...]), (planes + 2, high[2 * cols :, :])):
            for j, part in enumerate(strided_order(split(rows))):
                onsite[start : start + rows.shape[0], j * LANES : (j + 1) * LANES] = 6.0 + part
        for z in range(planes + 4):
            wide[z] = jnp.broadcast_to(onsite[z : z + 1, :], (cols, cells))

    inv_re, inv_im = inverses(onsite[...], nodes_ref[k, 0], nodes_ref[k, 1])
    for z in range(planes + 4):
        inv[0, z] = jnp.broadcast_to(inv_re[z : z + 1], (cols, cells))
        inv[1, z] = jnp.broadcast_to(inv_im[z : z + 1], (cols, cells))

    def at(j):
        return slice(j * LANES, (j + 1) * LANES)

    def factor(c, z, j):
        return inv[c, z, :, at(j)]

    for z in range(planes + 4):
        for j in range(vecs):
            value = b_ref[z, :, at(j)]
            u[0, z, :, at(j)] = value * factor(0, z, j)
            u[1, z, :, at(j)] = value * factor(1, z, j)

    def image(field, c, z):
        beside = plane_neighbours([field[c, z, :, at(j)] for j in range(vecs)])
        return [beside[j] + (field[c, z - 1, :, at(j)] + field[c, z + 1, :, at(j)]) for j in range(vecs)]

    outside = {0: where[1].astype(jnp.float32), planes + 1: where[2].astype(jnp.float32)}
    for z in range(planes + 2):
        real = image(u, 0, z + 1)
        imag = image(u, 1, z + 1)
        for j in range(vecs):
            re = b_ref[z + 1, :, at(j)] + real[j]
            im = imag[j]
            if z in outside:
                re = re * outside[z]
                im = im * outside[z]
            f_re = factor(0, z + 1, j)
            f_im = factor(1, z + 1, j)
            if z > 0:
                blocks[0, 0, z - 1, :, at(j)] = re
                blocks[0, 1, z - 1, :, at(j)] = im
            v[0, z, :, at(j)] = re * f_re - im * f_im
            v[1, z, :, at(j)] = re * f_im + im * f_re

    def accumulate(z, acc):
        real = image(v, 0, z + 1)
        imag = image(v, 1, z + 1)
        acc = list(acc)
        for j in range(vecs):
            re = blocks[0, 0, z, :, at(j)]
            im = blocks[0, 1, z, :, at(j)]
            two_re = re + real[j]
            two_im = im + imag[j]
            b = b_ref[z + 2, :, at(j)]
            acc[0] = acc[0] + (re * re + im * im)
            acc[1] = acc[1] + re * b
            acc[2] = acc[2] - im * b
            acc[3] = acc[3] + (re * two_re + im * two_im)
            acc[4] = acc[4] + (re * two_im - im * two_re)
            acc[5] = acc[5] + (two_re * two_re + two_im * two_im)
            acc[6] = acc[6] + two_re * b
            acc[7] = acc[7] - two_im * b
        return tuple(acc)

    zero = jnp.zeros((cols, LANES), jnp.float32)
    acc = (zero,) * PRODUCTS
    for z in range(planes):
        acc = accumulate(z, acc)
    lane = lane_iota(cols)
    total = sums[...]
    for i in range(PRODUCTS):
        total = jnp.where(lane == i * count + k, jnp.sum(acc[i], axis=1, keepdims=True), total)
    sums[...] = total


def moment_kernel(shifts, weights, blocks, b_ref, onsite, sums, out, coef):
    step = pl.program_id(0)
    nodes = blocks.shape[0]
    cols, cells = b_ref.shape[1:]
    vecs = cells // LANES

    @pl.when(step == 0)
    def _():
        total = sums[...]

        def of(i):
            return pltpu.roll(total, (LANES - i * nodes) % LANES, 1) if i else total

        g_one, q_one_re, q_one_im, g_mix_re, g_mix_im, g_two, q_two_re, q_two_im = map(of, range(PRODUCTS))
        ridge = RIDGE * (g_one + g_two) / 2.0
        determ = (g_one + ridge) * (g_two + ridge) - (g_mix_re * g_mix_re + g_mix_im * g_mix_im)
        one_re = ((g_two + ridge) * q_one_re - (g_mix_re * q_two_re - g_mix_im * q_two_im)) / determ
        one_im = ((g_two + ridge) * q_one_im - (g_mix_re * q_two_im + g_mix_im * q_two_re)) / determ
        two_re = ((g_one + ridge) * q_two_re - (g_mix_re * q_one_re + g_mix_im * q_one_im)) / determ
        two_im = ((g_one + ridge) * q_two_im - (g_mix_re * q_one_im - g_mix_im * q_one_re)) / determ
        w_re = weights[0:1, :]
        w_im = weights[1:2, :]
        scaled = (
            w_re * one_re - w_im * one_im,
            w_re * one_im + w_im * one_re,
            w_re * two_re - w_im * two_im,
            w_re * two_im + w_im * two_re,
        )
        for k in range(nodes):
            for i in range(4):
                coef[k, i] = jnp.broadcast_to(scaled[i][:, k : k + 1], (cols, LANES))

    for i in range(out.shape[0]):
        z = step * out.shape[0] + i
        result = []
        for j in range(vecs):
            at = slice(j * LANES, (j + 1) * LANES)
            b = b_ref[z + 2, :, at]
            total = jnp.zeros((cols, LANES), jnp.float32)
            inv_re, inv_im = inverses(onsite[z + 2, 0:1, at], shifts[0], shifts[1])
            for k in range(nodes):
                re = blocks[k, 0, i, :, at]
                im = blocks[k, 1, i, :, at]
                f_re = jnp.broadcast_to(inv_re[k : k + 1], (cols, LANES))
                f_im = jnp.broadcast_to(inv_im[k : k + 1], (cols, LANES))
                y_re = coef[k, 0] * b + coef[k, 2] * re - coef[k, 3] * im
                y_im = coef[k, 1] * b + coef[k, 3] * re + coef[k, 2] * im
                total = total + (f_re * y_re - f_im * y_im)
            result.append(total)
        for j, part in enumerate(natural_order(result)):
            out[i, :, j * LANES : (j + 1) * LANES] = part


def halves(x):
    high = x.astype(jnp.bfloat16)
    return high, (x - high.astype(jnp.float32)).astype(jnp.bfloat16)


def gram_kernel(where, pot, *refs, layout, scale):
    pieces, out, gram, edge = refs[: len(layout)], refs[-3], refs[-2], refs[-1]
    planes, width, cells = out.shape
    for ref, (mask, first) in zip(pieces, layout):
        cols = ref.shape[1]
        start = 0 if cols == width else pl.multiple_of((where[0] ^ mask) * cols, cols)
        for z in range(ref.shape[0]):
            if first + z < planes:
                out[first + z, pl.ds(start, cols), :] = ref[z]
            else:
                edge[pl.ds(start, cols), :] = ref[z]
    cell = lax.broadcasted_iota(jnp.int32, (1, cells), 1)
    x_ok = (cell < cells - NY).astype(jnp.float32)
    y_ok = (cell % NY != NY - 1).astype(jnp.float32)
    total = jnp.zeros((2 * width, 4 * width), jnp.float32)
    for z in range(planes):
        s = out[z]
        after = out[z + 1] if z + 1 < planes else edge[...]
        beside = pltpu.roll(s, cells - NY, 1) * x_ok + pltpu.roll(s, cells - 1, 1) * y_ok + after
        applied = (3.0 + 0.5 * pot[z : z + 1, :]) * s - beside
        s_high, s_low = halves(s)
        a_high, a_low = halves(applied)
        left = jnp.concatenate([s_high, s_low], axis=0)
        right = jnp.concatenate([a_high, s_high, a_low, s_low], axis=0)
        total = total + lax.dot_general(
            left, right, (((1,), (1,)), ((), ())), preferred_element_type=jnp.float32
        )
    both = total[:width, : 2 * width] + total[:width, 2 * width :] + total[width:, : 2 * width]
    gram[...] = both * scale


def butterfly(x, axis):
    count = lax.axis_size(axis)
    if count == 4:
        far = [lax.ppermute(x, axis, [(i, i ^ m) for i in range(4)]) for m in (2, 3, 1)]
        return (x + far[2]) + (far[0] + far[1])
    step = 1
    while step < count:
        x = x + lax.ppermute(x, axis, [(i, i ^ step) for i in range(count)])
        step *= 2
    return x


def swap(x, mask):
    count = lax.axis_size("shift")
    return lax.ppermute(x, "shift", [(i, i ^ mask) for i in range(count)])


def spread(x):
    count = lax.axis_size("shift")
    if x.shape[1] % 8:
        whole = lax.all_gather(x, "shift", axis=1)
        return [(0, 0, whole.reshape(x.shape[0], -1, x.shape[2]))]
    if count != 8:
        return [(0, 0, x)] + [(m, 0, swap(x, m)) for m in range(1, count)]
    half = x.shape[0] // 2
    a = swap(x, 2)
    b = swap(x, 4)
    d_first = swap(a[:half], 4)
    d_last = swap(b[half:], 2)
    held = [(0, 0, x), (2, 0, a), (4, 0, b), (6, 0, d_first), (6, half, d_last)]
    return held + [(m ^ 1, first, swap(piece, 1)) for m, first, piece in held]


def on_device(samples, potential):
    nodes = lax.axis_size("shift")
    slabs = lax.axis_size("dom")
    planes, width, cells = samples.shape
    cols = width // nodes
    me = lax.axis_index("shift")
    slab = lax.axis_index("dom")
    angles = [math.pi * (k + 0.5) / nodes for k in range(nodes)]
    table = np.array(
        [[CENTRE + RADIUS * math.cos(a), RADIUS * math.sin(a)] for a in angles], np.float32
    )
    shifts = np.ascontiguousarray(np.broadcast_to(table.T[:, :, None], (2, nodes, LANES)))
    spare = [0.0] * (LANES - nodes)
    weights = jnp.array(
        [
            [RADIUS * math.cos(a) / nodes for a in angles] + spare,
            [RADIUS * math.sin(a) / nodes for a in angles] + spare,
        ],
        jnp.float32,
    )
    where = jnp.stack([me, slab > 0, slab < slabs - 1, slab % 2 == 0]).astype(jnp.int32)

    def edge(start):
        part = lax.dynamic_slice(samples, (start, me * cols, 0), (2, cols, cells))
        rows = lax.dynamic_slice(potential, (start, 0), (2, cells))
        return jnp.concatenate([part.reshape(2 * cols, cells), rows], axis=0)

    def pairs(start):
        ups = [(i, i + 1) for i in range(start, slabs - 1, 2)]
        return ups + [(j, i) for i, j in ups]

    even = slab % 2 == 0
    paired = lax.ppermute(edge(jnp.where(even, planes - 2, 0)), "dom", pairs(0))
    other = lax.ppermute(edge(jnp.where(even, 0, planes - 2)), "dom", pairs(1))

    f32 = jnp.float32
    smem = pl.BlockSpec(memory_space=pltpu.SMEM)

    def full(shape):
        return pl.BlockSpec(shape, lambda *_: (0,) * len(shape))

    if cols % 8:
        source = lax.dynamic_slice_in_dim(samples, me * cols, cols, 1)
        own_spec = full(source.shape)
    else:
        source = samples
        own_spec = pl.BlockSpec((planes, cols, cells), lambda k, w: (0, w[0], 0))
    blocks, b_ext, onsite, sums = pl.pallas_call(
        krylov_kernel,
        grid_spec=pltpu.PrefetchScalarGridSpec(
            num_scalar_prefetch=1,
            grid=(nodes,),
            in_specs=[
                smem,
                own_spec,
                full(potential.shape),
                full(paired.shape),
                full(other.shape),
            ],
            out_specs=[
                pl.BlockSpec((1, 2, planes + 1, cols, cells), lambda k, w: (k, 0, 0, 0, 0)),
                full((planes + 4, cols, cells)),
                full((planes + 4, cols, cells)),
                full((cols, LANES)),
            ],
            scratch_shapes=[
                pltpu.VMEM((2, planes + 4, cols, cells), f32),
                pltpu.VMEM((2, planes + 2, cols, cells), f32),
                pltpu.VMEM((2, planes + 4, cols, cells), f32),
                pltpu.VMEM((planes + 4, cells), f32),
            ],
        ),
        out_shape=[
            jax.ShapeDtypeStruct((nodes, 2, planes + 1, cols, cells), f32),
            jax.ShapeDtypeStruct((planes + 4, cols, cells), f32),
            jax.ShapeDtypeStruct((planes + 4, cols, cells), f32),
            jax.ShapeDtypeStruct((cols, LANES), f32),
        ],
        name="krylov",
    )(where, table, source, potential, paired, other)

    totals = butterfly(sums, "dom")

    group = 3 if (planes + 1) % 3 == 0 else 1
    own = pl.pallas_call(
        moment_kernel,
        grid=((planes + 1) // group,),
        in_specs=[
            full(shifts.shape),
            full(weights.shape),
            pl.BlockSpec((nodes, 2, group, cols, cells), lambda z: (0, 0, z, 0, 0)),
            full(b_ext.shape),
            full(onsite.shape),
            full(totals.shape),
        ],
        out_specs=pl.BlockSpec((group, cols, cells), lambda z: (z, 0, 0)),
        out_shape=jax.ShapeDtypeStruct((planes + 1, cols, cells), f32),
        scratch_shapes=[
            pltpu.VMEM((nodes, 4, cols, LANES), f32),
        ],
        name="moment",
    )(shifts, weights, blocks, b_ext, onsite, totals)

    held = spread(own)
    layout = tuple((mask, first) for mask, first, _ in held)
    vmem = pl.BlockSpec(memory_space=pltpu.VMEM)
    scale = 1.0 / (cells * planes * slabs)
    subspace, gram = pl.pallas_call(
        functools.partial(gram_kernel, layout=layout, scale=scale),
        in_specs=[smem] + [vmem] * (1 + len(held)),
        out_specs=[vmem, vmem],
        out_shape=[
            jax.ShapeDtypeStruct((planes, width, cells), f32),
            jax.ShapeDtypeStruct((width, 2 * width), f32),
        ],
        scratch_shapes=[pltpu.VMEM((width, cells), f32)],
        name="gram",
    )(where, potential, *[piece for _, _, piece in held])
    gram = butterfly(gram, "dom")
    part_h = gram[:, :width]
    return subspace, part_h + part_h.T, gram[:, width:]


def solution(mesh):
    in_specs = (P("dom", None, None), P("dom", None))
    out_specs = (P("dom", None, None), P(), P())
    return jax.shard_map(
        on_device, mesh=mesh, in_specs=in_specs, out_specs=out_specs, check_vma=False
    )
```

```python
import functools
import math

import jax
import jax.numpy as jnp
import numpy as np
from jax import lax
from jax.experimental import pallas as pl
from jax.experimental.pallas import tpu as pltpu
from jax.sharding import PartitionSpec as P

NX = 32
NY = 32
LANES = 128


CENTRE = 3.0
RADIUS = 2.0
RIDGE = 0.01
PRODUCTS = 8


def lane_iota(rows):
    return lax.broadcasted_iota(jnp.int32, (rows, LANES), 1)


def split(ref_row):
    return [ref_row[:, j * LANES : (j + 1) * LANES] for j in range(ref_row.shape[-1] // LANES)]


def strided_order(parts):
    count = len(parts)
    blocks = LANES // NY
    lane_block = lane_iota(parts[0].shape[0]) // NY
    out = []
    for j in range(count):
        total = None
        for b in range(blocks):
            x = b * count + j
            turn = (NY * (b - x % blocks)) % LANES
            piece = parts[x // blocks]
            piece = pltpu.roll(piece, turn, 1) if turn else piece
            total = piece if total is None else jnp.where(lane_block == b, piece, total)
        out.append(total)
    return out


def natural_order(parts):
    count = len(parts)
    blocks = LANES // NY
    lane_block = lane_iota(parts[0].shape[0]) // NY
    out = []
    for v in range(count):
        total = None
        for c in range(blocks):
            x = v * blocks + c
            turn = (NY * (c - x // count)) % LANES
            piece = parts[x % count]
            piece = pltpu.roll(piece, turn, 1) if turn else piece
            total = piece if total is None else jnp.where(lane_block == c, piece, total)
        out.append(total)
    return out


def plane_neighbours(parts):
    count = len(parts)
    lane = lane_iota(parts[0].shape[0])
    has_low = (lane % NY != 0).astype(jnp.float32)
    has_high = (lane % NY != NY - 1).astype(jnp.float32)
    first = jnp.where(lane < NY, 0.0, pltpu.roll(parts[-1], NY, 1))
    last = jnp.where(lane >= LANES - NY, 0.0, pltpu.roll(parts[0], LANES - NY, 1))
    padded = [first] + parts + [last]
    return [
        padded[j] + padded[j + 2]
        + pltpu.roll(parts[j], 1, 1) * has_low
        + pltpu.roll(parts[j], LANES - 1, 1) * has_high
        for j in range(count)
    ]


def inverses(onsite, shift_re, shift_im):
    diag_re = shift_re - onsite
    scaled = 1.0 / (diag_re * diag_re + shift_im * shift_im)
    return diag_re * scaled, -shift_im * scaled


def krylov_kernel(where, node, own, pot, paired, other, blocks, b_ref, wide, sums, u, v, inv, onsite):
    k = pl.program_id(0)
    count = pl.num_programs(0)
    planes, cols, cells = own.shape
    vecs = cells // LANES

    @pl.when(k == 0)
    def _():
        sums[...] = jnp.zeros_like(sums)

        def put(z, parts):
            for j, part in enumerate(strided_order(parts)):
                b_ref[z, :, j * LANES : (j + 1) * LANES] = part

        even = where[3] > 0
        low = jnp.where(even, other[...], paired[...])
        high = jnp.where(even, paired[...], other[...])
        for i in range(2):
            put(i, split(low[i * cols : (i + 1) * cols, :]))
            put(planes + 2 + i, split(high[i * cols : (i + 1) * cols, :]))

        @pl.loop(0, planes)
        def _(z):
            put(z + 2, split(own[z]))

        for start, rows in ((0, low[2 * cols :, :]), (2, pot[...]), (planes + 2, high[2 * cols :, :])):
            for j, part in enumerate(strided_order(split(rows))):
                onsite[start : start + rows.shape[0], j * LANES : (j + 1) * LANES] = 6.0 + part
        for z in range(planes + 4):
            wide[z] = jnp.broadcast_to(onsite[z : z + 1, :], (cols, cells))

    def at(j):
        return slice(j * LANES, (j + 1) * LANES)

    for j in range(vecs):
        inv_re, inv_im = inverses(onsite[:, at(j)], node[0, 0:1, :], node[0, 1:2, :])
        for z in range(planes + 4):
            inv[0, z, :, at(j)] = jnp.broadcast_to(inv_re[z : z + 1], (cols, LANES))
            inv[1, z, :, at(j)] = jnp.broadcast_to(inv_im[z : z + 1], (cols, LANES))

    def factor(c, z, j):
        return inv[c, z, :, at(j)]

    for z in range(planes + 4):
        for j in range(vecs):
            value = b_ref[z, :, at(j)]
            u[0, z, :, at(j)] = value * factor(0, z, j)
            u[1, z, :, at(j)] = value * factor(1, z, j)

    def image(field, c, z):
        beside = plane_neighbours([field[c, z, :, at(j)] for j in range(vecs)])
        return [beside[j] + (field[c, z - 1, :, at(j)] + field[c, z + 1, :, at(j)]) for j in range(vecs)]

    outside = {0: where[1].astype(jnp.float32), planes + 1: where[2].astype(jnp.float32)}
    for z in range(planes + 2):
        real = image(u, 0, z + 1)
        imag = image(u, 1, z + 1)
        for j in range(vecs):
            re = b_ref[z + 1, :, at(j)] + real[j]
            im = imag[j]
            if z in outside:
                re = re * outside[z]
                im = im * outside[z]
            f_re = factor(0, z + 1, j)
            f_im = factor(1, z + 1, j)
            if z > 0:
                blocks[0, 0, z - 1, :, at(j)] = re
                blocks[0, 1, z - 1, :, at(j)] = im
            v[0, z, :, at(j)] = re * f_re - im * f_im
            v[1, z, :, at(j)] = re * f_im + im * f_re

    def accumulate(z, acc):
        real = image(v, 0, z + 1)
        imag = image(v, 1, z + 1)
        acc = list(acc)
        for j in range(vecs):
            re = blocks[0, 0, z, :, at(j)]
            im = blocks[0, 1, z, :, at(j)]
            two_re = re + real[j]
            two_im = im + imag[j]
            b = b_ref[z + 2, :, at(j)]
            acc[0] = acc[0] + (re * re + im * im)
            acc[1] = acc[1] + re * b
            acc[2] = acc[2] - im * b
            acc[3] = acc[3] + (re * two_re + im * two_im)
            acc[4] = acc[4] + (re * two_im - im * two_re)
            acc[5] = acc[5] + (two_re * two_re + two_im * two_im)
            acc[6] = acc[6] + two_re * b
            acc[7] = acc[7] - two_im * b
        return tuple(acc)

    zero = jnp.zeros((cols, LANES), jnp.float32)
    acc = (zero,) * PRODUCTS
    for z in range(planes):
        acc = accumulate(z, acc)
    lane = lane_iota(cols)
    total = sums[...]
    for i in range(PRODUCTS):
        total = jnp.where(lane == i * count + k, jnp.sum(acc[i], axis=1, keepdims=True), total)
    sums[...] = total


def moment_kernel(shifts, weights, blocks, b_ref, onsite, sums, out, coef):
    step = pl.program_id(0)
    nodes = blocks.shape[0]
    cols, cells = b_ref.shape[1:]
    vecs = cells // LANES

    @pl.when(step == 0)
    def _():
        total = sums[...]

        def of(i):
            return pltpu.roll(total, (LANES - i * nodes) % LANES, 1) if i else total

        g_one, q_one_re, q_one_im, g_mix_re, g_mix_im, g_two, q_two_re, q_two_im = map(of, range(PRODUCTS))
        ridge = RIDGE * (g_one + g_two) / 2.0
        determ = (g_one + ridge) * (g_two + ridge) - (g_mix_re * g_mix_re + g_mix_im * g_mix_im)
        one_re = ((g_two + ridge) * q_one_re - (g_mix_re * q_two_re - g_mix_im * q_two_im)) / determ
        one_im = ((g_two + ridge) * q_one_im - (g_mix_re * q_two_im + g_mix_im * q_two_re)) / determ
        two_re = ((g_one + ridge) * q_two_re - (g_mix_re * q_one_re + g_mix_im * q_one_im)) / determ
        two_im = ((g_one + ridge) * q_two_im - (g_mix_re * q_one_im - g_mix_im * q_one_re)) / determ
        w_re = weights[0:1, :]
        w_im = weights[1:2, :]
        scaled = (
            w_re * one_re - w_im * one_im,
            w_re * one_im + w_im * one_re,
            w_re * two_re - w_im * two_im,
            w_re * two_im + w_im * two_re,
        )
        for k in range(nodes):
            for i in range(4):
                coef[k, i] = jnp.broadcast_to(scaled[i][:, k : k + 1], (cols, LANES))

    for i in range(out.shape[0]):
        z = step * out.shape[0] + i
        result = []
        for j in range(vecs):
            at = slice(j * LANES, (j + 1) * LANES)
            b = b_ref[z + 2, :, at]
            total = jnp.zeros((cols, LANES), jnp.float32)
            inv_re, inv_im = inverses(onsite[z + 2, 0:1, at], shifts[0], shifts[1])
            for k in range(nodes):
                re = blocks[k, 0, i, :, at]
                im = blocks[k, 1, i, :, at]
                f_re = jnp.broadcast_to(inv_re[k : k + 1], (cols, LANES))
                f_im = jnp.broadcast_to(inv_im[k : k + 1], (cols, LANES))
                y_re = coef[k, 0] * b + coef[k, 2] * re - coef[k, 3] * im
                y_im = coef[k, 1] * b + coef[k, 3] * re + coef[k, 2] * im
                total = total + (f_re * y_re - f_im * y_im)
            result.append(total)
        for j, part in enumerate(natural_order(result)):
            out[i, :, j * LANES : (j + 1) * LANES] = part


def halves(x):
    high = x.astype(jnp.bfloat16)
    return high, (x - high.astype(jnp.float32)).astype(jnp.bfloat16)


def gram_kernel(where, pot, *refs, layout, scale):
    pieces = refs[: len(layout)]
    out, gram, field, sems = refs[len(layout) :]
    planes, width, cells = out.shape
    arrivals = []
    for i, (ref, (mask, first)) in enumerate(zip(pieces, layout)):
        count, cols = ref.shape[:2]
        start = 0 if cols == width else pl.multiple_of((where[0] ^ mask) * cols, cols)
        target = field.at[pl.ds(first, count), pl.ds(start, cols), :]
        arrivals.append(pltpu.make_async_copy(ref, target, sems.at[i]))
    for copy in arrivals:
        copy.start()
    for copy in arrivals:
        copy.wait()
    leave = pltpu.make_async_copy(field.at[pl.ds(0, planes)], out, sems.at[len(layout)])
    leave.start()
    cell = lax.broadcasted_iota(jnp.int32, (1, cells), 1)
    x_ok = (cell < cells - NY).astype(jnp.float32)
    y_ok = (cell % NY != NY - 1).astype(jnp.float32)
    total = jnp.zeros((2 * width, 4 * width), jnp.float32)
    for z in range(planes):
        s = field[z]
        after = field[z + 1]
        beside = pltpu.roll(s, cells - NY, 1) * x_ok + pltpu.roll(s, cells - 1, 1) * y_ok + after
        applied = (3.0 + 0.5 * pot[z : z + 1, :]) * s - beside
        s_high, s_low = halves(s)
        a_high, a_low = halves(applied)
        left = jnp.concatenate([s_high, s_low], axis=0)
        right = jnp.concatenate([a_high, s_high, a_low, s_low], axis=0)
        total = total + lax.dot_general(
            left, right, (((1,), (1,)), ((), ())), preferred_element_type=jnp.float32
        )
    both = total[:width, : 2 * width] + total[:width, 2 * width :] + total[width:, : 2 * width]
    both = both * scale
    half = both[:, :width]
    gram[:, :width] = half + half.T
    gram[:, width:] = both[:, width:]
    leave.wait()


def butterfly(x, axis):
    count = lax.axis_size(axis)
    if count == 4:
        far = [lax.ppermute(x, axis, [(i, i ^ m) for i in range(4)]) for m in (2, 3, 1)]
        return (x + far[2]) + (far[0] + far[1])
    step = 1
    while step < count:
        x = x + lax.ppermute(x, axis, [(i, i ^ step) for i in range(count)])
        step *= 2
    return x


def swap(x, mask):
    count = lax.axis_size("shift")
    return lax.ppermute(x, "shift", [(i, i ^ mask) for i in range(count)])


def spread(x):
    count = lax.axis_size("shift")
    if x.shape[1] % 8:
        whole = lax.all_gather(x, "shift", axis=1)
        return [(0, 0, whole.reshape(x.shape[0], -1, x.shape[2]))]
    if count != 8:
        return [(0, 0, x)] + [(m, 0, swap(x, m)) for m in range(1, count)]
    half = x.shape[0] // 2
    a = swap(x, 2)
    b = swap(x, 4)
    d_first = swap(a[:half], 4)
    d_last = swap(b[half:], 2)
    held = [(0, 0, x), (2, 0, a), (4, 0, b), (6, 0, d_first), (6, half, d_last)]
    return held + [(m ^ 1, first, swap(piece, 1)) for m, first, piece in held]


def on_device(samples, potential):
    nodes = lax.axis_size("shift")
    slabs = lax.axis_size("dom")
    planes, width, cells = samples.shape
    cols = width // nodes
    me = lax.axis_index("shift")
    slab = lax.axis_index("dom")
    angles = [math.pi * (k + 0.5) / nodes for k in range(nodes)]
    table = np.array(
        [[CENTRE + RADIUS * math.cos(a), RADIUS * math.sin(a)] for a in angles], np.float32
    )
    shifts = np.ascontiguousarray(np.broadcast_to(table.T[:, :, None], (2, nodes, LANES)))
    rows = np.ascontiguousarray(np.broadcast_to(table[:, :, None], (nodes, 2, LANES)))
    spare = [0.0] * (LANES - nodes)
    weights = jnp.array(
        [
            [RADIUS * math.cos(a) / nodes for a in angles] + spare,
            [RADIUS * math.sin(a) / nodes for a in angles] + spare,
        ],
        jnp.float32,
    )
    where = jnp.stack([me, slab > 0, slab < slabs - 1, slab % 2 == 0]).astype(jnp.int32)

    def edge(start):
        part = lax.dynamic_slice(samples, (start, me * cols, 0), (2, cols, cells))
        rows = lax.dynamic_slice(potential, (start, 0), (2, cells))
        return jnp.concatenate([part.reshape(2 * cols, cells), rows], axis=0)

    def pairs(start):
        ups = [(i, i + 1) for i in range(start, slabs - 1, 2)]
        return ups + [(j, i) for i, j in ups]

    even = slab % 2 == 0
    paired = lax.ppermute(edge(jnp.where(even, planes - 2, 0)), "dom", pairs(0))
    other = lax.ppermute(edge(jnp.where(even, 0, planes - 2)), "dom", pairs(1))

    f32 = jnp.float32
    smem = pl.BlockSpec(memory_space=pltpu.SMEM)

    def full(shape):
        return pl.BlockSpec(shape, lambda *_: (0,) * len(shape))

    if cols % 8:
        source = lax.dynamic_slice_in_dim(samples, me * cols, cols, 1)
        own_spec = full(source.shape)
    else:
        source = samples
        own_spec = pl.BlockSpec((planes, cols, cells), lambda k, w: (0, w[0], 0))
    blocks, b_ext, onsite, sums = pl.pallas_call(
        krylov_kernel,
        grid_spec=pltpu.PrefetchScalarGridSpec(
            num_scalar_prefetch=1,
            grid=(nodes,),
            in_specs=[
                pl.BlockSpec((1, 2, LANES), lambda k, w: (k, 0, 0)),
                own_spec,
                full(potential.shape),
                full(paired.shape),
                full(other.shape),
            ],
            out_specs=[
                pl.BlockSpec((1, 2, planes + 1, cols, cells), lambda k, w: (k, 0, 0, 0, 0)),
                full((planes + 4, cols, cells)),
                full((planes + 4, cols, cells)),
                full((cols, LANES)),
            ],
            scratch_shapes=[
                pltpu.VMEM((2, planes + 4, cols, cells), f32),
                pltpu.VMEM((2, planes + 2, cols, cells), f32),
                pltpu.VMEM((2, planes + 4, cols, cells), f32),
                pltpu.VMEM((planes + 4, cells), f32),
            ],
        ),
        out_shape=[
            jax.ShapeDtypeStruct((nodes, 2, planes + 1, cols, cells), f32),
            jax.ShapeDtypeStruct((planes + 4, cols, cells), f32),
            jax.ShapeDtypeStruct((planes + 4, cols, cells), f32),
            jax.ShapeDtypeStruct((cols, LANES), f32),
        ],
        name="krylov",
    )(where, rows, source, potential, paired, other)

    totals = butterfly(sums, "dom")

    group = 3 if (planes + 1) % 3 == 0 else 1
    own = pl.pallas_call(
        moment_kernel,
        grid=((planes + 1) // group,),
        in_specs=[
            full(shifts.shape),
            full(weights.shape),
            pl.BlockSpec((nodes, 2, group, cols, cells), lambda z: (0, 0, z, 0, 0)),
            full(b_ext.shape),
            full(onsite.shape),
            full(totals.shape),
        ],
        out_specs=pl.BlockSpec((group, cols, cells), lambda z: (z, 0, 0)),
        out_shape=jax.ShapeDtypeStruct((planes + 1, cols, cells), f32),
        scratch_shapes=[
            pltpu.VMEM((nodes, 4, cols, LANES), f32),
        ],
        name="moment",
    )(shifts, weights, blocks, b_ext, onsite, totals)

    held = spread(own)
    layout = tuple((mask, first) for mask, first, _ in held)
    vmem = pl.BlockSpec(memory_space=pltpu.VMEM)
    hbm = pl.BlockSpec(memory_space=pl.ANY)
    scale = 1.0 / (cells * planes * slabs)
    subspace, gram = pl.pallas_call(
        functools.partial(gram_kernel, layout=layout, scale=scale),
        in_specs=[smem, vmem] + [hbm] * len(held),
        out_specs=[hbm, vmem],
        out_shape=[
            jax.ShapeDtypeStruct((planes, width, cells), f32),
            jax.ShapeDtypeStruct((width, 2 * width), f32),
        ],
        scratch_shapes=[
            pltpu.VMEM((planes + 1, width, cells), f32),
            pltpu.SemaphoreType.DMA((len(held) + 1,)),
        ],
        name="gram",
    )(where, potential, *[piece for _, _, piece in held])
    gram = butterfly(gram, "dom")
    return subspace, gram[:, :width], gram[:, width:]


def solution(mesh):
    in_specs = (P("dom", None, None), P("dom", None))
    out_specs = (P("dom", None, None), P(), P())
    return jax.shard_map(
        on_device, mesh=mesh, in_specs=in_specs, out_specs=out_specs, check_vma=False
    )
```

```python
import functools
import math

import jax
import jax.numpy as jnp
import numpy as np
from jax import lax
from jax.experimental import pallas as pl
from jax.experimental.pallas import tpu as pltpu
from jax.sharding import PartitionSpec as P

NX = 32
NY = 32
LANES = 128


CENTRE = 3.0
RADIUS = 2.0
RIDGE = 0.01
PRODUCTS = 8


def lane_iota(rows):
    return lax.broadcasted_iota(jnp.int32, (rows, LANES), 1)


def split(ref_row):
    return [ref_row[:, j * LANES : (j + 1) * LANES] for j in range(ref_row.shape[-1] // LANES)]


def strided_order(parts):
    count = len(parts)
    blocks = LANES // NY
    lane_block = lane_iota(parts[0].shape[0]) // NY
    out = []
    for j in range(count):
        total = None
        for b in range(blocks):
            x = b * count + j
            turn = (NY * (b - x % blocks)) % LANES
            piece = parts[x // blocks]
            piece = pltpu.roll(piece, turn, 1) if turn else piece
            total = piece if total is None else jnp.where(lane_block == b, piece, total)
        out.append(total)
    return out


def natural_order(parts):
    count = len(parts)
    blocks = LANES // NY
    lane_block = lane_iota(parts[0].shape[0]) // NY
    out = []
    for v in range(count):
        total = None
        for c in range(blocks):
            x = v * blocks + c
            turn = (NY * (c - x // count)) % LANES
            piece = parts[x % count]
            piece = pltpu.roll(piece, turn, 1) if turn else piece
            total = piece if total is None else jnp.where(lane_block == c, piece, total)
        out.append(total)
    return out


def plane_neighbours(parts):
    count = len(parts)
    lane = lane_iota(parts[0].shape[0])
    has_low = (lane % NY != 0).astype(jnp.float32)
    has_high = (lane % NY != NY - 1).astype(jnp.float32)
    first = jnp.where(lane < NY, 0.0, pltpu.roll(parts[-1], NY, 1))
    last = jnp.where(lane >= LANES - NY, 0.0, pltpu.roll(parts[0], LANES - NY, 1))
    padded = [first] + parts + [last]
    return [
        padded[j] + padded[j + 2]
        + pltpu.roll(parts[j], 1, 1) * has_low
        + pltpu.roll(parts[j], LANES - 1, 1) * has_high
        for j in range(count)
    ]


def inverses(onsite, shift_re, shift_im):
    diag_re = shift_re - onsite
    scaled = 1.0 / (diag_re * diag_re + shift_im * shift_im)
    return diag_re * scaled, -shift_im * scaled


def krylov_kernel(where, node, own, pot, paired, other, blocks, b_ref, wide, sums, u, v, inv, onsite):
    k = pl.program_id(0)
    count = pl.num_programs(0)
    planes, cols, cells = own.shape
    vecs = cells // LANES

    @pl.when(k == 0)
    def _():
        sums[...] = jnp.zeros_like(sums)

        def put(z, parts):
            for j, part in enumerate(strided_order(parts)):
                b_ref[z, :, j * LANES : (j + 1) * LANES] = part

        even = where[3] > 0
        low = jnp.where(even, other[...], paired[...])
        high = jnp.where(even, paired[...], other[...])
        for i in range(2):
            put(i, split(low[i * cols : (i + 1) * cols, :]))
            put(planes + 2 + i, split(high[i * cols : (i + 1) * cols, :]))

        @pl.loop(0, planes)
        def _(z):
            put(z + 2, split(own[z]))

        for start, rows in ((0, low[2 * cols :, :]), (2, pot[...]), (planes + 2, high[2 * cols :, :])):
            for j, part in enumerate(strided_order(split(rows))):
                onsite[start : start + rows.shape[0], j * LANES : (j + 1) * LANES] = 6.0 + part
        for z in range(planes + 4):
            wide[z] = jnp.broadcast_to(onsite[z : z + 1, :], (cols, cells))

    def at(j):
        return slice(j * LANES, (j + 1) * LANES)

    for j in range(vecs):
        inv_re, inv_im = inverses(onsite[:, at(j)], node[0, 0:1, :], node[0, 1:2, :])
        for z in range(planes + 4):
            inv[0, z, :, at(j)] = jnp.broadcast_to(inv_re[z : z + 1], (cols, LANES))
            inv[1, z, :, at(j)] = jnp.broadcast_to(inv_im[z : z + 1], (cols, LANES))

    def factor(c, z, j):
        return inv[c, z, :, at(j)]

    for z in range(planes + 4):
        for j in range(vecs):
            value = b_ref[z, :, at(j)]
            u[0, z, :, at(j)] = value * factor(0, z, j)
            u[1, z, :, at(j)] = value * factor(1, z, j)

    def image(field, c, z):
        beside = plane_neighbours([field[c, z, :, at(j)] for j in range(vecs)])
        return [beside[j] + (field[c, z - 1, :, at(j)] + field[c, z + 1, :, at(j)]) for j in range(vecs)]

    outside = {0: where[1].astype(jnp.float32), planes + 1: where[2].astype(jnp.float32)}
    for z in range(planes + 2):
        real = image(u, 0, z + 1)
        imag = image(u, 1, z + 1)
        for j in range(vecs):
            re = b_ref[z + 1, :, at(j)] + real[j]
            im = imag[j]
            if z in outside:
                re = re * outside[z]
                im = im * outside[z]
            f_re = factor(0, z + 1, j)
            f_im = factor(1, z + 1, j)
            if z > 0:
                blocks[0, 0, z - 1, :, at(j)] = re
                blocks[0, 1, z - 1, :, at(j)] = im
            v[0, z, :, at(j)] = re * f_re - im * f_im
            v[1, z, :, at(j)] = re * f_im + im * f_re

    def accumulate(z, acc):
        real = image(v, 0, z + 1)
        imag = image(v, 1, z + 1)
        acc = list(acc)
        for j in range(vecs):
            re = blocks[0, 0, z, :, at(j)]
            im = blocks[0, 1, z, :, at(j)]
            two_re = re + real[j]
            two_im = im + imag[j]
            b = b_ref[z + 2, :, at(j)]
            acc[0] = acc[0] + (re * re + im * im)
            acc[1] = acc[1] + re * b
            acc[2] = acc[2] - im * b
            acc[3] = acc[3] + (re * two_re + im * two_im)
            acc[4] = acc[4] + (re * two_im - im * two_re)
            acc[5] = acc[5] + (two_re * two_re + two_im * two_im)
            acc[6] = acc[6] + two_re * b
            acc[7] = acc[7] - two_im * b
        return tuple(acc)

    zero = jnp.zeros((cols, LANES), jnp.float32)
    acc = (zero,) * PRODUCTS
    for z in range(planes):
        acc = accumulate(z, acc)
    lane = lane_iota(cols)
    total = sums[...]
    for i in range(PRODUCTS):
        total = jnp.where(lane == i * count + k, jnp.sum(acc[i], axis=1, keepdims=True), total)
    sums[...] = total


def moment_kernel(shifts, weights, blocks, b_ref, onsite, sums, out, coef):
    step = pl.program_id(0)
    nodes = blocks.shape[0]
    cols, cells = b_ref.shape[1:]
    vecs = cells // LANES

    @pl.when(step == 0)
    def _():
        total = sums[...]

        def of(i):
            return pltpu.roll(total, (LANES - i * nodes) % LANES, 1) if i else total

        g_one, q_one_re, q_one_im, g_mix_re, g_mix_im, g_two, q_two_re, q_two_im = map(of, range(PRODUCTS))
        ridge = RIDGE * (g_one + g_two) / 2.0
        determ = (g_one + ridge) * (g_two + ridge) - (g_mix_re * g_mix_re + g_mix_im * g_mix_im)
        one_re = ((g_two + ridge) * q_one_re - (g_mix_re * q_two_re - g_mix_im * q_two_im)) / determ
        one_im = ((g_two + ridge) * q_one_im - (g_mix_re * q_two_im + g_mix_im * q_two_re)) / determ
        two_re = ((g_one + ridge) * q_two_re - (g_mix_re * q_one_re + g_mix_im * q_one_im)) / determ
        two_im = ((g_one + ridge) * q_two_im - (g_mix_re * q_one_im - g_mix_im * q_one_re)) / determ
        w_re = weights[0:1, :]
        w_im = weights[1:2, :]
        scaled = (
            w_re * one_re - w_im * one_im,
            w_re * one_im + w_im * one_re,
            w_re * two_re - w_im * two_im,
            w_re * two_im + w_im * two_re,
        )
        for k in range(nodes):
            for i in range(4):
                coef[k, i] = jnp.broadcast_to(scaled[i][:, k : k + 1], (cols, LANES))

    for i in range(out.shape[0]):
        z = step * out.shape[0] + i
        result = []
        for j in range(vecs):
            at = slice(j * LANES, (j + 1) * LANES)
            b = b_ref[z + 2, :, at]
            total = jnp.zeros((cols, LANES), jnp.float32)
            inv_re, inv_im = inverses(onsite[z + 2, 0:1, at], shifts[0], shifts[1])
            for k in range(nodes):
                re = blocks[k, 0, i, :, at]
                im = blocks[k, 1, i, :, at]
                f_re = jnp.broadcast_to(inv_re[k : k + 1], (cols, LANES))
                f_im = jnp.broadcast_to(inv_im[k : k + 1], (cols, LANES))
                y_re = coef[k, 0] * b + coef[k, 2] * re - coef[k, 3] * im
                y_im = coef[k, 1] * b + coef[k, 3] * re + coef[k, 2] * im
                total = total + (f_re * y_re - f_im * y_im)
            result.append(total)
        for j, part in enumerate(natural_order(result)):
            out[i, :, j * LANES : (j + 1) * LANES] = part


def halves(x):
    high = x.astype(jnp.bfloat16)
    return high, (x - high.astype(jnp.float32)).astype(jnp.bfloat16)


def gram_kernel(where, pot, *refs, layout, scale):
    pieces = refs[: len(layout)]
    out, gram, field, sems = refs[len(layout) :]
    planes, width, cells = out.shape
    arrivals = []
    for i, (ref, (mask, first)) in enumerate(zip(pieces, layout)):
        count, cols = ref.shape[:2]
        start = 0 if cols == width else pl.multiple_of((where[0] ^ mask) * cols, cols)
        target = field.at[pl.ds(first, count), pl.ds(start, cols), :]
        arrivals.append(pltpu.make_async_copy(ref, target, sems.at[i]))
    for copy in arrivals:
        copy.start()
    for copy in arrivals:
        copy.wait()
    leave = pltpu.make_async_copy(field.at[pl.ds(0, planes)], out, sems.at[len(layout)])
    leave.start()
    cell = lax.broadcasted_iota(jnp.int32, (1, cells), 1)
    x_ok = (cell < cells - NY).astype(jnp.float32)
    y_ok = (cell % NY != NY - 1).astype(jnp.float32)
    total = jnp.zeros((2 * width, 4 * width), jnp.float32)
    for z in range(planes):
        s = field[z]
        after = field[z + 1]
        beside = pltpu.roll(s, cells - NY, 1) * x_ok + pltpu.roll(s, cells - 1, 1) * y_ok + after
        applied = (3.0 + 0.5 * pot[z : z + 1, :]) * s - beside
        s_high, s_low = halves(s)
        a_high, a_low = halves(applied)
        left = jnp.concatenate([s_high, s_low], axis=0)
        right = jnp.concatenate([a_high, s_high, a_low, s_low], axis=0)
        total = total + lax.dot_general(
            left, right, (((1,), (1,)), ((), ())), preferred_element_type=jnp.float32
        )
    both = total[:width, : 2 * width] + total[:width, 2 * width :] + total[width:, : 2 * width]
    both = both * scale
    half = both[:, :width]
    gram[:, :width] = half + half.T
    gram[:, width:] = both[:, width:]
    leave.wait()


def butterfly(x, axis):
    count = lax.axis_size(axis)
    if count == 4:
        far = [lax.ppermute(x, axis, [(i, i ^ m) for i in range(4)]) for m in (2, 3, 1)]
        return (x + far[2]) + (far[0] + far[1])
    step = 1
    while step < count:
        x = x + lax.ppermute(x, axis, [(i, i ^ step) for i in range(count)])
        step *= 2
    return x


def swap(x, mask):
    count = lax.axis_size("shift")
    return lax.ppermute(x, "shift", [(i, i ^ mask) for i in range(count)])


def spread(x):
    count = lax.axis_size("shift")
    if x.shape[1] % 8:
        whole = lax.all_gather(x, "shift", axis=1)
        return [(0, 0, whole.reshape(x.shape[0], -1, x.shape[2]))]
    if count != 8:
        return [(0, 0, x)] + [(m, 0, swap(x, m)) for m in range(1, count)]
    half = x.shape[0] // 2
    a = swap(x, 2)
    b = swap(x, 4)
    d_first = swap(a[:half], 4)
    d_last = swap(b[half:], 2)
    held = [(0, 0, x), (2, 0, a), (4, 0, b), (6, 0, d_first), (6, half, d_last)]
    return held + [(m ^ 1, first, swap(piece, 1)) for m, first, piece in held]


def on_device(samples, potential):
    nodes = lax.axis_size("shift")
    slabs = lax.axis_size("dom")
    planes, width, cells = samples.shape
    cols = width // nodes
    me = lax.axis_index("shift")
    slab = lax.axis_index("dom")
    angles = [math.pi * (k + 0.5) / nodes for k in range(nodes)]
    table = np.array(
        [[CENTRE + RADIUS * math.cos(a), RADIUS * math.sin(a)] for a in angles], np.float32
    )
    shifts = np.ascontiguousarray(np.broadcast_to(table.T[:, :, None], (2, nodes, LANES)))
    rows = np.ascontiguousarray(np.broadcast_to(table[:, :, None], (nodes, 2, LANES)))
    spare = [0.0] * (LANES - nodes)
    weights = jnp.array(
        [
            [RADIUS * math.cos(a) / nodes for a in angles] + spare,
            [RADIUS * math.sin(a) / nodes for a in angles] + spare,
        ],
        jnp.float32,
    )
    where = jnp.stack([me, slab > 0, slab < slabs - 1, slab % 2 == 0]).astype(jnp.int32)

    def edge(start):
        part = lax.dynamic_slice(samples, (start, me * cols, 0), (2, cols, cells))
        rows = lax.dynamic_slice(potential, (start, 0), (2, cells))
        return jnp.concatenate([part.reshape(2 * cols, cells), rows], axis=0)

    def pairs(start):
        ups = [(i, i + 1) for i in range(start, slabs - 1, 2)]
        return ups + [(j, i) for i, j in ups]

    even = slab % 2 == 0
    paired = lax.ppermute(edge(jnp.where(even, planes - 2, 0)), "dom", pairs(0))
    other = lax.ppermute(edge(jnp.where(even, 0, planes - 2)), "dom", pairs(1))

    f32 = jnp.float32
    smem = pl.BlockSpec(memory_space=pltpu.SMEM)

    def full(shape):
        return pl.BlockSpec(shape, lambda *_: (0,) * len(shape))

    if cols % 8:
        source = lax.dynamic_slice_in_dim(samples, me * cols, cols, 1)
        own_spec = full(source.shape)
    else:
        source = samples
        own_spec = pl.BlockSpec((planes, cols, cells), lambda k, w: (0, w[0], 0))
    blocks, b_ext, onsite, sums = pl.pallas_call(
        krylov_kernel,
        grid_spec=pltpu.PrefetchScalarGridSpec(
            num_scalar_prefetch=1,
            grid=(nodes,),
            in_specs=[
                pl.BlockSpec((1, 2, LANES), lambda k, w: (k, 0, 0)),
                own_spec,
                full(potential.shape),
                full(paired.shape),
                full(other.shape),
            ],
            out_specs=[
                pl.BlockSpec((1, 2, planes + 1, cols, cells), lambda k, w: (k, 0, 0, 0, 0)),
                full((planes + 4, cols, cells)),
                full((planes + 4, cols, cells)),
                full((cols, LANES)),
            ],
            scratch_shapes=[
                pltpu.VMEM((2, planes + 4, cols, cells), f32),
                pltpu.VMEM((2, planes + 2, cols, cells), f32),
                pltpu.VMEM((2, planes + 4, cols, cells), f32),
                pltpu.VMEM((planes + 4, cells), f32),
            ],
        ),
        out_shape=[
            jax.ShapeDtypeStruct((nodes, 2, planes + 1, cols, cells), f32),
            jax.ShapeDtypeStruct((planes + 4, cols, cells), f32),
            jax.ShapeDtypeStruct((planes + 4, cols, cells), f32),
            jax.ShapeDtypeStruct((cols, LANES), f32),
        ],
        name="krylov",
    )(where, rows, source, potential, paired, other)

    totals = butterfly(sums, "dom")

    group = 3 if (planes + 1) % 3 == 0 else 1
    own = pl.pallas_call(
        moment_kernel,
        grid=((planes + 1) // group,),
        in_specs=[
            full(shifts.shape),
            full(weights.shape),
            pl.BlockSpec((nodes, 2, group, cols, cells), lambda z: (0, 0, z, 0, 0)),
            full(b_ext.shape),
            full(onsite.shape),
            full(totals.shape),
        ],
        out_specs=pl.BlockSpec((group, cols, cells), lambda z: (z, 0, 0)),
        out_shape=jax.ShapeDtypeStruct((planes + 1, cols, cells), f32),
        scratch_shapes=[
            pltpu.VMEM((nodes, 4, cols, LANES), f32),
        ],
        name="moment",
    )(shifts, weights, blocks, b_ext, onsite, totals)

    held = spread(own)
    layout = tuple((mask, first) for mask, first, _ in held)
    vmem = pl.BlockSpec(memory_space=pltpu.VMEM)
    hbm = pl.BlockSpec(memory_space=pltpu.HBM)
    scale = 1.0 / (cells * planes * slabs)
    subspace, gram = pl.pallas_call(
        functools.partial(gram_kernel, layout=layout, scale=scale),
        in_specs=[smem, vmem] + [hbm] * len(held),
        out_specs=[hbm, vmem],
        out_shape=[
            jax.ShapeDtypeStruct((planes, width, cells), f32),
            jax.ShapeDtypeStruct((width, 2 * width), f32),
        ],
        scratch_shapes=[
            pltpu.VMEM((planes + 1, width, cells), f32),
            pltpu.SemaphoreType.DMA((len(held) + 1,)),
        ],
        name="gram",
    )(where, potential, *[piece for _, _, piece in held])
    gram = butterfly(gram, "dom")
    return subspace, gram[:, :width], gram[:, width:]


def solution(mesh):
    in_specs = (P("dom", None, None), P("dom", None))
    out_specs = (P("dom", None, None), P(), P())
    return jax.shard_map(
        on_device, mesh=mesh, in_specs=in_specs, out_specs=out_specs, check_vma=False
    )
```
